32 devices in a mesh: seg: 32 (over z, y, x, core).
Axes of the slice: x: 2, y: 2, z: 4, core: 2. Of those that a mesh axis runs over, the one named last changes fastest.
Arguments:
- strain: bfloat16 [3, 64, 3, 2, 65536], P(None, 'seg'), may hold values from -6 to 6
- valid: int32 [64], P('seg'), may hold values from 0 to 1, as said below
- intersection: float32 [3, 65536], replicated, may hold values from -1 to 1, as said below
- notch: int32 [65536], replicated, may hold values from 0 to 1, as said below
Outputs:
- contribution: float32 [3, 65536], P(None, 'seg')
- broadband: float32 [3, 2], replicated
The draws below stay inside these ranges and needn't reach their ends.
Inputs may be any that keep to these rules, and one draw needn't show every extreme that they name: At least one segment is valid. `intersection`: never zero. `notch`: at least one bin is kept.
All inputs are finite; a program needn't handle non-finite values.
Results may differ from the reference program's by a relative error of at most 0.011.
Values sent between devices are 32-bit elements; how exact they have to be, the bound alone decides.
No kernel may reach another device: no remote copies, remote signals or barrier semaphores. Data moves between devices by JAX's collectives and lax.ppermute only.
A program may use at most 256 MiB of HBM per device.

```python
import math
import jax
import jax.numpy as jnp
from jax import lax

FA = 256
FB = 256
STR = 3
SEGMENTS = 64


def draw_valid(key, part):
    marks = jax.random.randint(jax.random.fold_in(key, 11), (SEGMENTS,), 0, 4)
    forced = jax.random.randint(jax.random.fold_in(key, 12), (), 0, SEGMENTS)
    flags = jnp.where(marks > 0, 1, 0)
    flags = jnp.where(jnp.arange(SEGMENTS) == forced, 1, flags)
    return flags.astype(jnp.int32)


def draw_notch(key, part):
    marks = jax.random.randint(jax.random.fold_in(key, 21), (FA * FB,), 0, 10)
    forced = jax.random.randint(jax.random.fold_in(key, 22), (), 0, FA * FB)
    flags = jnp.where(marks > 0, 1, 0)
    flags = jnp.where(jnp.arange(FA * FB) == forced, 1, flags)
    return flags.astype(jnp.int32)


def draw_intersection(key, part):
    position = jnp.arange(FA * FB, dtype=jnp.float32)[None, :] / (FA * FB)
    signs = jax.random.randint(jax.random.fold_in(key, 31), (3, FA * FB), 0, 2)
    signs = jnp.where(signs > 0, 1.0, -1.0)
    rough = jax.random.uniform(jax.random.fold_in(key, 33), (3, FA * FB), jnp.float32, 0.3, 1.0)
    shape = jnp.exp(-1.5 * position)
    return (signs * rough * shape).astype(jnp.float32)


def block_scale(key, shape, shards, low, high):
    def one(dim, parts):
        steps = jax.random.uniform(jax.random.fold_in(jax.random.fold_in(key, 6), dim), (parts,), jnp.float32, low / len(shards), high / len(shards))
        return jnp.repeat(jnp.exp(steps), shape[dim] // parts).reshape((-1,) + (1,) * (len(shape) - dim - 1))

    loudness = one(*shards[0])
    for cut in shards[1:]:
        loudness = loudness * one(*cut)
    return loudness


def normal_values(stream_key, shape, width, bound, shards=(), kind=jnp.bfloat16):
    drawn = width * jax.random.normal(stream_key, shape, jnp.float32)
    if shards:
        drawn = drawn * block_scale(stream_key, shape, shards, -0.22, 0.18)
    return jnp.clip(drawn, -bound, bound).astype(kind)


def setup_inputs(seed: int = 0) -> dict:
    key_of = jax.random.split(jax.random.key(seed), 5)
    return {
        "strain": normal_values(key_of[0], (3, SEGMENTS, STR, 2, FA * FB), 1.0, 6.0, ((1, 32),)),
        "valid": draw_valid(jax.random.fold_in(key_of[4], 71), 0),
        "intersection": draw_intersection(jax.random.fold_in(key_of[4], 71), 0),
        "notch": draw_notch(jax.random.fold_in(key_of[4], 71), 0),
    }


baseline_pairs = ((0, 1), (0, 2), (1, 2))

def dft_tables(length):
    counter = jnp.arange(length, dtype=jnp.int32)
    phases = counter[:, None] * counter[None, :] % length
    angles = phases.astype(jnp.float32) * (2.0 * math.pi / length)
    return (jnp.cos(angles).astype(jnp.bfloat16), jnp.sin(angles).astype(jnp.bfloat16))

def twiddle(rows, cols):
    phases = jnp.arange(rows, dtype=jnp.int32)[:, None] * jnp.arange(cols, dtype=jnp.int32)[None, :]
    angles = phases.astype(jnp.float32) * (2.0 * math.pi / (rows * cols))
    return (jnp.cos(angles), jnp.sin(angles))

def mult(table, data, form):
    return jnp.einsum(form, table.astype(jnp.float32), data.astype(jnp.float32))

def spectra(strain, rows, cols):
    lead = strain.shape[:3]
    real_in = strain[:, :, :, 0].reshape(-1, rows, cols)
    imag_in = strain[:, :, :, 1].reshape(-1, rows, cols)
    cos_rows, sin_rows = dft_tables(rows)
    first_real = mult(cos_rows, real_in, 'kn,bnq->bkq') + mult(sin_rows, imag_in, 'kn,bnq->bkq')
    first_imag = mult(cos_rows, imag_in, 'kn,bnq->bkq') - mult(sin_rows, real_in, 'kn,bnq->bkq')
    tw_cos, tw_sin = twiddle(rows, cols)
    mid_real = (first_real * tw_cos + first_imag * tw_sin).astype(jnp.bfloat16)
    mid_imag = (first_imag * tw_cos - first_real * tw_sin).astype(jnp.bfloat16)
    cos_cols, sin_cols = dft_tables(cols)
    last_real = mult(cos_cols, mid_real, 'kn,bpn->bkp') + mult(sin_cols, mid_imag, 'kn,bpn->bkp')
    last_imag = mult(cos_cols, mid_imag, 'kn,bpn->bkp') - mult(sin_cols, mid_real, 'kn,bpn->bkp')
    scale = 1.0 / math.sqrt(rows * cols)
    shape = lead + (rows * cols,)
    return (last_real.reshape(shape) * scale, last_imag.reshape(shape) * scale)

def segment_stats(real_part, imag_part, valid_float):
    power = lax.optimization_barrier(jnp.mean(real_part * real_part + imag_part * imag_part, axis=2))
    weights = []
    weighted = []
    for first, second in baseline_pairs:
        cross = lax.optimization_barrier(jnp.mean(real_part[first] * real_part[second] + imag_part[first] * imag_part[second], axis=1))
        weight = valid_float[:, None] / (power[first] * power[second])
        weights.append(weight)
        weighted.append(weight * cross)
    return jnp.stack(weights + weighted, axis=1)

def reference(strain, valid, intersection, notch):

    def step(carry, index):
        piece = lax.dynamic_slice_in_dim(strain, index, 1, 1)
        flags = lax.dynamic_slice_in_dim(valid, index, 1, 0).astype(jnp.float32)
        real_part, imag_part = spectra(piece, FA, FB)
        return (carry + segment_stats(real_part, imag_part, flags)[0], None)
    start = jnp.zeros((6, FA * FB), jnp.float32)
    sums, _ = lax.scan(step, start, jnp.arange(SEGMENTS, dtype=jnp.int32))
    weight_sum = sums[:3]
    numer = sums[3:]
    kept = notch.astype(jnp.float32)[None, :]
    signal = lax.optimization_barrier(jnp.sum(kept * intersection * numer, axis=1))
    info = lax.optimization_barrier(jnp.sum(kept * intersection * intersection * weight_sum, axis=1))
    contribution = kept * intersection * numer / jnp.sqrt(info / (FA * FB))[:, None]
    broadband = jnp.stack([signal / jnp.sqrt(info), jnp.sqrt(info / (FA * FB))], axis=1)
    return (contribution, broadband)
```

```python
import functools
import math

import jax
import jax.numpy as jnp
import numpy as np
from jax import lax
from jax.experimental import pallas as pl
from jax.experimental.pallas import tpu as pltpu
from jax.sharding import PartitionSpec as P

FA = 256
FB = 256
LANES = 128
BLOCK = 16
GROUP = 8


baseline_pairs = ((0, 1), (0, 2), (1, 2))


def dft_table(length):
    counter = np.arange(length)
    angles = (counter[:, None] * counter[None, :] % length).astype(np.float32) * np.float32(2.0 * math.pi / length)
    cos, sin = np.cos(angles), np.sin(angles)
    real = np.concatenate([cos, sin], axis=1).reshape(-1, BLOCK, 2 * length)
    imag = np.concatenate([-sin, cos], axis=1).reshape(-1, BLOCK, 2 * length)
    return jnp.asarray(np.stack([real, imag], axis=1).reshape(2 * length, 2 * length), jnp.bfloat16)


def twiddle(rows, cols):
    phases = np.arange(rows)[:, None] * np.arange(cols)[None, :]
    angles = phases.astype(np.float32) * np.float32(2.0 * math.pi / (rows * cols))
    scale = np.float32(1.0 / math.sqrt(rows * cols))
    return jnp.asarray(np.stack([np.cos(angles) * scale, np.sin(angles) * scale]), jnp.float32)


def kernel(dets, segs, strs, valid_ref, x_hbm, table_hbm, tw_hbm, inter_ref, notch_ref, out_ref,
           xs, table, tw, wide, mid, spec, stats, sem, table_sem):
    trips = segs * strs
    loads = {}
    def load(f):
        return pltpu.make_async_copy(x_hbm.at[f], xs.at[f], sem.at[f])
    table_load = pltpu.make_async_copy(table_hbm, table, table_sem.at[0])
    tw_load = pltpu.make_async_copy(tw_hbm, tw, table_sem.at[1])
    for d in range(dets):
        load(d * trips).start()
    table_load.start()
    tw_load.start()
    for i in range(1, trips):
        for d in range(dets):
            load(d * trips + i).start()

    def spectrum(d, i):
        f = d * trips + i
        load(f).wait()
        wide[d] = xs[f].astype(jnp.float32)
        cols = []
        for h in range(2):
            parts = [wide[d, pl.ds(2 * h + c, FA, stride=4), :] for c in range(2)]
            cols.append(jnp.concatenate(parts, axis=0).astype(jnp.bfloat16))
        data = jnp.concatenate(cols, axis=1)
        first = jnp.dot(table[...], data, preferred_element_type=jnp.float32)
        for r in range(FA // BLOCK):
            rows = pl.ds(r * BLOCK, BLOCK)
            real = first[2 * r * BLOCK:(2 * r + 1) * BLOCK]
            imag = first[(2 * r + 1) * BLOCK:(2 * r + 2) * BLOCK]
            u, v = tw[0, rows, :], tw[1, rows, :]
            mid[d, rows, :FB] = (real * u + imag * v).astype(jnp.bfloat16)
            mid[d, rows, FB:] = (imag * u - real * v).astype(jnp.bfloat16)
        spec[d] = lax.dot_general(table[...], mid[d], (((1,), (1,)), ((), ())),
                                  preferred_element_type=jnp.float32)

    def add_stats(start):
        for r in range(FB // BLOCK):
            rows = pl.ds(r * BLOCK, BLOCK)
            real = [spec[d, pl.ds(2 * r * BLOCK, BLOCK), :] for d in range(dets)]
            imag = [spec[d, pl.ds((2 * r + 1) * BLOCK, BLOCK), :] for d in range(dets)]
            pairs = [(d, d) for d in range(dets)] + list(baseline_pairs)
            for n, (i, j) in enumerate(pairs):
                value = real[i] * real[j] + imag[i] * imag[j]
                stats[n, rows, :] = value if start else stats[n, rows, :] + value

    nb = len(baseline_pairs)
    sums = [jnp.zeros((GROUP, LANES), jnp.float32) for _ in range(2 * nb)]
    table_load.wait()
    tw_load.wait()
    for s in range(segs):
        for d in range(dets):
            spectrum(d, s * strs)
        add_stats(True)

        @pl.loop(1, strs)
        def _(t):
            for d in range(dets):
                spectrum(d, s * strs + t)
            add_stats(False)

        flag = valid_ref[s].astype(jnp.float32)

        def combine(g, sums):
            sums = list(sums)
            for h in range(FA // LANES):
                lanes = pl.ds(h * LANES, LANES)
                rows = pl.ds(pl.multiple_of(g * GROUP, GROUP), GROUP)
                bins = pl.ds(g * GROUP * 2 + h, GROUP, stride=2)
                kept = notch_ref[bins, :].astype(jnp.float32)
                power = [stats[d, rows, lanes] for d in range(dets)]
                for b, (i, j) in enumerate(baseline_pairs):
                    slot = pl.ds((b * 2 + h) * GROUP, GROUP)
                    weight = flag / (power[i] * power[j])
                    numer = weight * stats[dets + b, rows, lanes]
                    inter = inter_ref[b, bins, :]
                    scaled = kept * inter
                    sums[b] = sums[b] + scaled * inter * weight
                    sums[nb + b] = sums[nb + b] + scaled * numer
                    if s == 0:
                        out_ref[g, slot, :] = numer
                    else:
                        out_ref[g, slot, :] = out_ref[g, slot, :] + numer
            return tuple(sums)

        sums = lax.fori_loop(0, FB // GROUP, combine, tuple(sums))
    tail = jnp.concatenate([jnp.sum(v, axis=0, keepdims=True) for v in sums]
                           + [jnp.zeros((GROUP - 2 * nb, LANES), jnp.float32)], axis=0)
    for g in range(FB // GROUP):
        out_ref[g, pl.ds(2 * nb * GROUP, GROUP), :] = tail


def local_sums(strain, valid, intersection, notch):
    dets, segs, strs = strain.shape[:3]
    halves = FB // LANES
    x = strain.reshape(dets * segs * strs, 2, FA, halves, LANES).transpose(0, 2, 3, 1, 4)
    x = x.reshape(dets * segs * strs, 2 * FA * halves, LANES)
    inter = intersection.reshape(len(baseline_pairs), -1, LANES)
    kept = notch.reshape(-1, LANES)
    count = x.shape[0]
    rows = 2 * len(baseline_pairs) * GROUP + GROUP
    any_spec = pl.BlockSpec(memory_space=pl.ANY)
    vmem = pl.BlockSpec(memory_space=pltpu.VMEM)
    return pl.pallas_call(
        functools.partial(kernel, dets, segs, strs),
        out_shape=jax.ShapeDtypeStruct((FB // GROUP, rows, LANES), jnp.float32),
        in_specs=[pl.BlockSpec(memory_space=pltpu.SMEM), any_spec, any_spec, any_spec, vmem, vmem],
        out_specs=vmem,
        scratch_shapes=[
            pltpu.VMEM((count, 2 * FA * halves, LANES), jnp.bfloat16),
            pltpu.VMEM((2 * FA, 2 * FA), jnp.bfloat16),
            pltpu.VMEM((2, FA, FB), jnp.float32),
            pltpu.VMEM((dets, 2 * FA * halves, LANES), jnp.float32),
            pltpu.VMEM((dets, FA, 2 * FB), jnp.bfloat16),
            pltpu.VMEM((dets, 2 * FB, FA), jnp.float32),
            pltpu.VMEM((dets + len(baseline_pairs), FB, FA), jnp.float32),
            pltpu.SemaphoreType.DMA((count,)),
            pltpu.SemaphoreType.DMA((2,)),
        ],
        cost_estimate=pl.CostEstimate(flops=count * 16 * FA * FA * FB, bytes_accessed=2 * x.size,
                                      transcendentals=0),
    )(valid, x, dft_table(FA), twiddle(FA, FB), inter, kept)


def exchange(x, devices):
    me = lax.axis_index("seg")
    base = 1
    while base < devices:
        radix = 2 if base == 1 or devices // base % 4 else 4
        x = x.reshape((-1, radix) + x.shape[1:])
        digit = me // base % radix
        total = lax.dynamic_index_in_dim(x, digit, 1, keepdims=False)
        for k in range(1, radix):
            sent = lax.dynamic_index_in_dim(x, digit ^ k, 1, keepdims=False)
            total = total + lax.ppermute(sent, "seg", [(i, i ^ (k * base)) for i in range(devices)])
        x = total
        base *= radix
    return x[0]


def local(strain, valid, intersection, notch):
    total_bins = intersection.shape[1]
    devices = lax.axis_size("seg")
    local_bins = total_bins // devices
    pairs = len(baseline_pairs)
    strs = strain.shape[2]
    halves = FA // LANES
    x = local_sums(strain, valid, intersection, notch)
    own = local_bins // FA
    if own != GROUP:
        numer = x[:, :pairs * halves * GROUP].reshape(-1, pairs, halves, GROUP, LANES)
        numer = numer.transpose(1, 2, 0, 3, 4).reshape(pairs, halves, devices, own, LANES)
        numer = numer.transpose(2, 0, 1, 3, 4).reshape(devices, pairs * halves * own, LANES)
        tail = jnp.broadcast_to(x[:1, pairs * halves * GROUP:], (devices, GROUP, LANES))
        x = jnp.concatenate([numer, tail], axis=1)
    x = exchange(x, devices)
    size = pairs * halves * own
    numer = x[:size].reshape(pairs, halves, own, LANES).transpose(0, 2, 1, 3).reshape(pairs, local_bins)
    totals = jnp.sum(x[size:size + 2 * pairs], axis=1)
    info = totals[:pairs] * (strs * strs)
    signal = totals[pairs:] * strs
    start = lax.axis_index("seg") * local_bins
    inter = lax.dynamic_slice_in_dim(intersection, start, local_bins, 1)
    kept = lax.dynamic_slice_in_dim(notch, start, local_bins, 0).astype(jnp.float32)[None, :]
    contribution = kept * inter * (numer * strs) / jnp.sqrt(info / total_bins)[:, None]
    broadband = jnp.stack([signal / jnp.sqrt(info), jnp.sqrt(info / total_bins)], axis=1)
    return (contribution, broadband)


def solution(mesh):
    in_specs = (P(None, "seg", None, None, None), P("seg"), P(), P())
    out_specs = (P(None, "seg"), P())
    return jax.shard_map(local, mesh=mesh, in_specs=in_specs, out_specs=out_specs, check_vma=False)
```

```python
import functools
import math

import jax
import jax.numpy as jnp
import numpy as np
from jax import lax
from jax.experimental import pallas as pl
from jax.experimental.pallas import tpu as pltpu
from jax.sharding import PartitionSpec as P

FA = 256
FB = 256
LANES = 128
BLOCK = 16
GROUP = 8


baseline_pairs = ((0, 1), (0, 2), (1, 2))


def dft_table(length):
    counter = np.arange(length)
    angles = (counter[:, None] * counter[None, :] % length).astype(np.float32) * np.float32(2.0 * math.pi / length)
    cos, sin = np.cos(angles), np.sin(angles)
    real = np.concatenate([cos, sin], axis=1).reshape(-1, BLOCK, 2 * length)
    imag = np.concatenate([-sin, cos], axis=1).reshape(-1, BLOCK, 2 * length)
    return jnp.asarray(np.stack([real, imag], axis=1).reshape(2 * length, 2 * length), jnp.bfloat16)


def twiddle(rows, cols):
    phases = np.arange(rows)[:, None] * np.arange(cols)[None, :]
    angles = phases.astype(np.float32) * np.float32(2.0 * math.pi / (rows * cols))
    scale = np.float32(1.0 / math.sqrt(rows * cols))
    return jnp.asarray(np.stack([np.cos(angles) * scale, np.sin(angles) * scale]), jnp.float32)


def kernel(dets, segs, strs, valid_hbm, x_hbm, table_hbm, tw_hbm, inter_hbm, notch_hbm, out_ref,
           valid_ref, xs, table, tw, inter, notch, wide, mid, spec, stats, sem, table_sem):
    trips = segs * strs
    nb = len(baseline_pairs)

    def load(i):
        part = pl.ds(0, 1) if i == 0 else pl.ds(1, trips - 1)
        return pltpu.make_async_copy(x_hbm.at[:, part], xs.at[:, part], sem.at[i])

    others = [pltpu.make_async_copy(a, b, table_sem.at[n]) for n, (a, b) in enumerate(
        [(table_hbm, table), (tw_hbm, tw), (inter_hbm, inter), (notch_hbm, notch), (valid_hbm, valid_ref)])]
    load(0).start()
    for copy in others[:2]:
        copy.start()
    for i in range(1, 2):
        load(i).start()
    for copy in others[2:]:
        copy.start()

    def spectrum(d, i):
        wide[d] = xs[d, i].astype(jnp.float32)
        cols = []
        for h in range(2):
            parts = [wide[d, pl.ds(2 * h + c, FA, stride=4), :] for c in range(2)]
            cols.append(jnp.concatenate(parts, axis=0).astype(jnp.bfloat16))
        data = jnp.concatenate(cols, axis=1)
        first = jnp.dot(table[...], data, preferred_element_type=jnp.float32)
        for r in range(FA // BLOCK):
            rows = pl.ds(r * BLOCK, BLOCK)
            real = first[2 * r * BLOCK:(2 * r + 1) * BLOCK]
            imag = first[(2 * r + 1) * BLOCK:(2 * r + 2) * BLOCK]
            u, v = tw[0, rows, :], tw[1, rows, :]
            mid[d, rows, :FB] = (real * u + imag * v).astype(jnp.bfloat16)
            mid[d, rows, FB:] = (imag * u - real * v).astype(jnp.bfloat16)
        spec[i % 2, d] = lax.dot_general(table[...], mid[d], (((1,), (1,)), ((), ())),
                                         preferred_element_type=jnp.float32)

    def add_stats(i, part):
        s, t = i // strs, i % strs
        for r in range(part * FB // BLOCK // dets, (part + 1) * FB // BLOCK // dets):
            rows = pl.ds(r * BLOCK, BLOCK)
            real = [spec[i % 2, d, pl.ds(2 * r * BLOCK, BLOCK), :] for d in range(dets)]
            imag = [spec[i % 2, d, pl.ds((2 * r + 1) * BLOCK, BLOCK), :] for d in range(dets)]
            pairs = [(d, d) for d in range(dets)] + list(baseline_pairs)
            for n, (j, k) in enumerate(pairs):
                value = real[j] * real[k] + imag[j] * imag[k]
                stats[s, n, rows, :] = value if t == 0 else stats[s, n, rows, :] + value

    for i in range(trips):
        if i < 2:
            load(i).wait()
        if i == 0:
            for copy in others[:2]:
                copy.wait()
        for d in range(dets):
            spectrum(d, i)
            if i:
                add_stats(i - 1, d)
    for d in range(dets):
        add_stats(trips - 1, d)
    for copy in others[2:]:
        copy.wait()
    flags = [valid_ref[s].astype(jnp.float32) for s in range(segs)]

    def combine(g, sums):
        sums = list(sums)
        for h in range(FA // LANES):
            lanes = pl.ds(h * LANES, LANES)
            rows = pl.ds(pl.multiple_of(g * GROUP, GROUP), GROUP)
            bins = pl.ds(g * GROUP * 2 + h, GROUP, stride=2)
            kept = notch[bins, :].astype(jnp.float32)
            power = [[stats[s, d, rows, lanes] for d in range(dets)] for s in range(segs)]
            for b, (i, j) in enumerate(baseline_pairs):
                weights = [flags[s] / (power[s][i] * power[s][j]) for s in range(segs)]
                numer = weights[0] * stats[0, dets + b, rows, lanes]
                weight = weights[0]
                for s in range(1, segs):
                    numer = numer + weights[s] * stats[s, dets + b, rows, lanes]
                    weight = weight + weights[s]
                scaled = kept * inter[bins, b, :]
                sums[b] = sums[b] + scaled * inter[bins, b, :] * weight
                sums[nb + b] = sums[nb + b] + scaled * numer
                out_ref[g, pl.ds((b * 2 + h) * GROUP, GROUP), :] = numer
        return tuple(sums)

    sums = lax.fori_loop(0, FB // GROUP, combine,
                         tuple(jnp.zeros((GROUP, LANES), jnp.float32) for _ in range(2 * nb)))
    tail = jnp.concatenate([jnp.sum(v, axis=0, keepdims=True) for v in sums]
                           + [jnp.zeros((GROUP - 2 * nb, LANES), jnp.float32)], axis=0)
    for g in range(FB // GROUP):
        out_ref[g, pl.ds(2 * nb * GROUP, GROUP), :] = tail


def local_sums(strain, valid, intersection, notch):
    dets, segs, strs = strain.shape[:3]
    halves = FB // LANES
    x = strain.reshape(dets * segs * strs, 2, FA, halves, LANES).transpose(0, 2, 3, 1, 4)
    x = x.reshape(dets, segs * strs, 2 * FA * halves, LANES)
    inter = intersection.reshape(len(baseline_pairs), -1, LANES).transpose(1, 0, 2)
    kept = notch.reshape(-1, LANES)
    count = dets * segs * strs
    rows = 2 * len(baseline_pairs) * GROUP + GROUP
    any_spec = pl.BlockSpec(memory_space=pl.ANY)
    vmem = pl.BlockSpec(memory_space=pltpu.VMEM)
    return pl.pallas_call(
        functools.partial(kernel, dets, segs, strs),
        out_shape=jax.ShapeDtypeStruct((FB // GROUP, rows, LANES), jnp.float32),
        in_specs=[any_spec] * 6,
        out_specs=vmem,
        scratch_shapes=[
            pltpu.SMEM(valid.shape, jnp.int32),
            pltpu.VMEM(x.shape, jnp.bfloat16),
            pltpu.VMEM((2 * FA, 2 * FA), jnp.bfloat16),
            pltpu.VMEM((2, FA, FB), jnp.float32),
            pltpu.VMEM(inter.shape, jnp.float32),
            pltpu.VMEM(kept.shape, jnp.int32),
            pltpu.VMEM((dets, 2 * FA * halves, LANES), jnp.float32),
            pltpu.VMEM((dets, FA, 2 * FB), jnp.bfloat16),
            pltpu.VMEM((2, dets, 2 * FB, FA), jnp.float32),
            pltpu.VMEM((segs, dets + len(baseline_pairs), FB, FA), jnp.float32),
            pltpu.SemaphoreType.DMA((count,)),
            pltpu.SemaphoreType.DMA((5,)),
        ],
        compiler_params=pltpu.CompilerParams(vmem_limit_bytes=30 << 20),
        cost_estimate=pl.CostEstimate(flops=count * 16 * FA * FA * FB, bytes_accessed=2 * x.size,
                                      transcendentals=0),
    )(*(pltpu.with_memory_space_constraint(v, pltpu.HBM) for v in (valid, x, dft_table(FA), twiddle(FA, FB), inter, kept)))


def exchange(x, devices, me):
    base = 1
    terms = [x]
    while base < devices:
        radix = 2 if base == 1 or devices // base % 4 else 4
        x = functools.reduce(jnp.add, terms)
        x = x.reshape((-1, radix) + x.shape[1:])
        digit = jnp.bitwise_and(lax.shift_right_logical(me, base.bit_length() - 1), radix - 1)
        terms = [lax.dynamic_index_in_dim(x, digit, 1, keepdims=False)]
        for k in range(1, radix):
            sent = lax.dynamic_index_in_dim(x, jnp.bitwise_xor(digit, k), 1, keepdims=False)
            terms.append(lax.ppermute(sent, "seg", [(i, i ^ (k * base)) for i in range(devices)]))
        base *= radix
    return [v[0] for v in terms]


def finish_kernel(own, strs, total_bins, count, *refs):
    terms, (scaled_ref, contribution_ref, broadband_ref) = refs[:count], refs[count:]
    pairs = len(baseline_pairs)
    halves = FA // LANES
    size = pairs * halves * own
    x = functools.reduce(jnp.add, [ref[...] for ref in terms])
    totals = jnp.sum(x[size:size + 2 * pairs], axis=1, keepdims=True)
    for b in range(pairs):
        info = totals[b:b + 1] * (strs * strs)
        signal = totals[pairs + b:pairs + b + 1] * strs
        root = jnp.sqrt(info / total_bins)
        for h in range(halves):
            slot = pl.ds((b * halves + h) * own, own)
            value = scaled_ref[slot, :] * (x[slot.start:slot.start + own] * strs) / root
            for q in range(own):
                contribution_ref[b:b + 1, pl.ds(q * FA + h * LANES, LANES)] = value[q:q + 1]
        broadband_ref[0:1, b:b + 1] = signal / jnp.sqrt(info)
        broadband_ref[1:2, b:b + 1] = root


def local(strain, valid, intersection, notch):
    total_bins = intersection.shape[1]
    devices = lax.axis_size("seg")
    me = lax.axis_index("seg")
    local_bins = total_bins // devices
    pairs = len(baseline_pairs)
    halves = FA // LANES
    own = local_bins // FA
    start = me * local_bins
    inter = lax.dynamic_slice_in_dim(intersection, start, local_bins, 1)
    kept = lax.dynamic_slice_in_dim(notch, start, local_bins, 0).astype(jnp.float32)[None, :]
    scaled = (kept * inter).reshape(pairs, own, halves, LANES).transpose(0, 2, 1, 3)
    scaled = scaled.reshape(pairs * halves * own, LANES)
    x = local_sums(strain, valid, intersection, notch)
    if own != GROUP:
        numer = x[:, :pairs * halves * GROUP].reshape(-1, pairs, halves, GROUP, LANES)
        numer = numer.transpose(1, 2, 0, 3, 4).reshape(pairs, halves, devices, own, LANES)
        numer = numer.transpose(2, 0, 1, 3, 4).reshape(devices, pairs * halves * own, LANES)
        tail = jnp.broadcast_to(x[:1, pairs * halves * GROUP:], (devices, GROUP, LANES))
        x = jnp.concatenate([numer, tail], axis=1)
    terms = exchange(x, devices, me)
    contribution, broadband = pl.pallas_call(
        functools.partial(finish_kernel, own, strain.shape[2], total_bins, len(terms)),
        out_shape=(jax.ShapeDtypeStruct((pairs, local_bins), jnp.float32),
                   jax.ShapeDtypeStruct((2, pairs), jnp.float32)),
        compiler_params=pltpu.CompilerParams(vmem_limit_bytes=4 << 20),
    )(*terms, scaled)
    return (contribution, broadband.T)


def solution(mesh):
    in_specs = (P(None, "seg", None, None, None), P("seg"), P(), P())
    out_specs = (P(None, "seg"), P())
    return jax.shard_map(local, mesh=mesh, in_specs=in_specs, out_specs=out_specs, check_vma=False)
```

```python
import functools
import math

import jax
import jax.numpy as jnp
import numpy as np
from jax import lax
from jax.experimental import pallas as pl
from jax.experimental.pallas import tpu as pltpu
from jax.sharding import PartitionSpec as P

FA = 256
FB = 256
LANES = 128
BLOCK = 16
GROUP = 8


baseline_pairs = ((0, 1), (0, 2), (1, 2))


def dft_table(length):
    counter = np.arange(length)
    angles = (counter[:, None] * counter[None, :] % length).astype(np.float32) * np.float32(2.0 * math.pi / length)
    cos, sin = np.cos(angles), np.sin(angles)
    real = np.concatenate([cos, sin], axis=1).reshape(-1, BLOCK, 2 * length)
    imag = np.concatenate([-sin, cos], axis=1).reshape(-1, BLOCK, 2 * length)
    return jnp.asarray(np.stack([real, imag], axis=1).reshape(2 * length, 2 * length), jnp.bfloat16)


def twiddle(rows, cols):
    phases = np.arange(rows)[:, None] * np.arange(cols)[None, :]
    angles = phases.astype(np.float32) * np.float32(2.0 * math.pi / (rows * cols))
    scale = np.float32(1.0 / math.sqrt(rows * cols))
    return jnp.asarray(np.stack([np.cos(angles) * scale, np.sin(angles) * scale]), jnp.float32)


def kernel(dets, segs, strs, valid_hbm, x_hbm, table_hbm, tw_hbm, inter_hbm, notch_hbm, out_ref, tail_ref,
           valid_ref, xs, table, tw, inter, notch, wide, mid, spec, stats, sem, table_sem):
    trips = segs * strs
    nb = len(baseline_pairs)

    def load(i):
        part = pl.ds(0, 1) if i == 0 else pl.ds(1, trips - 1)
        return pltpu.make_async_copy(x_hbm.at[:, part], xs.at[:, part], sem.at[i])

    others = [pltpu.make_async_copy(a, b, table_sem.at[n]) for n, (a, b) in enumerate(
        [(table_hbm, table), (tw_hbm, tw), (inter_hbm, inter), (notch_hbm, notch), (valid_hbm, valid_ref)])]
    load(0).start()
    for copy in others[:2]:
        copy.start()
    for i in range(1, 2):
        load(i).start()
    for copy in others[2:]:
        copy.start()

    def spectrum(d, i):
        wide[d] = xs[d, i].astype(jnp.float32)
        cols = []
        for h in range(2):
            parts = [wide[d, pl.ds(2 * h + c, FA, stride=4), :] for c in range(2)]
            cols.append(jnp.concatenate(parts, axis=0).astype(jnp.bfloat16))
        data = jnp.concatenate(cols, axis=1)
        first = jnp.dot(table[...], data, preferred_element_type=jnp.float32)
        for r in range(FA // BLOCK):
            rows = pl.ds(r * BLOCK, BLOCK)
            real = first[2 * r * BLOCK:(2 * r + 1) * BLOCK]
            imag = first[(2 * r + 1) * BLOCK:(2 * r + 2) * BLOCK]
            u, v = tw[0, rows, :], tw[1, rows, :]
            mid[d, rows, :FB] = (real * u + imag * v).astype(jnp.bfloat16)
            mid[d, rows, FB:] = (imag * u - real * v).astype(jnp.bfloat16)
        spec[i % 2, d] = lax.dot_general(table[...], mid[d], (((1,), (1,)), ((), ())),
                                         preferred_element_type=jnp.float32)

    def add_stats(i, part):
        s, t = i // strs, i % strs
        for r in range(part * FB // BLOCK // dets, (part + 1) * FB // BLOCK // dets):
            rows = pl.ds(r * BLOCK, BLOCK)
            real = [spec[i % 2, d, pl.ds(2 * r * BLOCK, BLOCK), :] for d in range(dets)]
            imag = [spec[i % 2, d, pl.ds((2 * r + 1) * BLOCK, BLOCK), :] for d in range(dets)]
            pairs = [(d, d) for d in range(dets)] + list(baseline_pairs)
            for n, (j, k) in enumerate(pairs):
                value = real[j] * real[k] + imag[j] * imag[k]
                stats[s, n, rows, :] = value if t == 0 else stats[s, n, rows, :] + value

    for i in range(trips):
        if i < 2:
            load(i).wait()
        if i == 0:
            for copy in others[:2]:
                copy.wait()
        for d in range(dets):
            spectrum(d, i)
            if i:
                add_stats(i - 1, d)
    for d in range(dets):
        add_stats(trips - 1, d)
    for copy in others[2:]:
        copy.wait()
    flags = [valid_ref[s].astype(jnp.float32) for s in range(segs)]

    def combine(g, sums):
        sums = list(sums)
        for h in range(FA // LANES):
            lanes = pl.ds(h * LANES, LANES)
            rows = pl.ds(pl.multiple_of(g * GROUP, GROUP), GROUP)
            bins = pl.ds(g * GROUP * 2 + h, GROUP, stride=2)
            kept = notch[bins, :].astype(jnp.float32)
            power = [[stats[s, d, rows, lanes] for d in range(dets)] for s in range(segs)]
            for b, (i, j) in enumerate(baseline_pairs):
                weights = [flags[s] / (power[s][i] * power[s][j]) for s in range(segs)]
                numer = weights[0] * stats[0, dets + b, rows, lanes]
                weight = weights[0]
                for s in range(1, segs):
                    numer = numer + weights[s] * stats[s, dets + b, rows, lanes]
                    weight = weight + weights[s]
                scaled = kept * inter[bins, b, :]
                sums[b] = sums[b] + scaled * inter[bins, b, :] * weight
                sums[nb + b] = sums[nb + b] + scaled * numer
                out_ref[g, pl.ds((b * 2 + h) * GROUP, GROUP), :] = numer
        return tuple(sums)

    sums = lax.fori_loop(0, FB // GROUP, combine,
                         tuple(jnp.zeros((GROUP, LANES), jnp.float32) for _ in range(2 * nb)), unroll=4)
    tail = jnp.concatenate([jnp.sum(v, axis=0, keepdims=True) for v in sums]
                           + [jnp.zeros((GROUP - 2 * nb, LANES), jnp.float32)], axis=0)
    tail_ref[...] = tail


def local_sums(strain, valid, intersection, notch):
    dets, segs, strs = strain.shape[:3]
    halves = FB // LANES
    x = strain.reshape(dets * segs * strs, 2, FA, halves, LANES).transpose(0, 2, 3, 1, 4)
    x = x.reshape(dets, segs * strs, 2 * FA * halves, LANES)
    inter = intersection.reshape(len(baseline_pairs), -1, LANES).transpose(1, 0, 2)
    kept = notch.reshape(-1, LANES)
    count = dets * segs * strs
    rows = 2 * len(baseline_pairs) * GROUP
    any_spec = pl.BlockSpec(memory_space=pl.ANY)
    vmem = pl.BlockSpec(memory_space=pltpu.VMEM)
    return pl.pallas_call(
        functools.partial(kernel, dets, segs, strs),
        out_shape=(jax.ShapeDtypeStruct((FB // GROUP, rows, LANES), jnp.float32),
                   jax.ShapeDtypeStruct((GROUP, LANES), jnp.float32)),
        in_specs=[any_spec] * 6,
        out_specs=(vmem, vmem),
        scratch_shapes=[
            pltpu.SMEM(valid.shape, jnp.int32),
            pltpu.VMEM(x.shape, jnp.bfloat16),
            pltpu.VMEM((2 * FA, 2 * FA), jnp.bfloat16),
            pltpu.VMEM((2, FA, FB), jnp.float32),
            pltpu.VMEM(inter.shape, jnp.float32),
            pltpu.VMEM(kept.shape, jnp.int32),
            pltpu.VMEM((dets, 2 * FA * halves, LANES), jnp.float32),
            pltpu.VMEM((dets, FA, 2 * FB), jnp.bfloat16),
            pltpu.VMEM((2, dets, 2 * FB, FA), jnp.float32),
            pltpu.VMEM((segs, dets + len(baseline_pairs), FB, FA), jnp.float32),
            pltpu.SemaphoreType.DMA((count,)),
            pltpu.SemaphoreType.DMA((5,)),
        ],
        compiler_params=pltpu.CompilerParams(vmem_limit_bytes=30 << 20),
        cost_estimate=pl.CostEstimate(flops=count * 16 * FA * FA * FB, bytes_accessed=2 * x.size,
                                      transcendentals=0),
    )(*(pltpu.with_memory_space_constraint(v, pltpu.HBM) for v in (valid, x, dft_table(FA), twiddle(FA, FB), inter, kept)))


def exchange(x, tail, devices, me):
    base = 1
    total = jnp.concatenate([x.reshape(-1, LANES), tail])
    count = devices
    while base < devices:
        radix = 2 if base == 1 or devices // base % 4 else 4
        count //= radix
        size = tail.shape[0]
        parts, tail = total[:-size].reshape(count, radix, -1, LANES), total[-size:]
        digit = jnp.bitwise_and(lax.shift_right_logical(me, base.bit_length() - 1), radix - 1)

        def part(k):
            own = lax.dynamic_index_in_dim(parts, jnp.bitwise_xor(digit, k), 1, keepdims=False)
            return jnp.concatenate([own.reshape(-1, LANES), tail])

        terms = [part(0)] + [lax.ppermute(part(k), "seg", [(i, i ^ (k * base)) for i in range(devices)])
                             for k in range(radix - 1, 0, -1)]
        total = functools.reduce(jnp.add, terms)
        base *= radix
    return terms


def finish_kernel(own, strs, total_bins, count, *refs):
    terms, (scaled_ref, contribution_ref, broadband_ref) = refs[:count], refs[count:]
    pairs = len(baseline_pairs)
    halves = FA // LANES
    size = pairs * halves * own
    x = functools.reduce(jnp.add, [ref[...] for ref in terms])
    totals = jnp.sum(x[size:size + 2 * pairs], axis=1, keepdims=True)
    for b in range(pairs):
        info = totals[b:b + 1] * (strs * strs)
        signal = totals[pairs + b:pairs + b + 1] * strs
        root = jnp.sqrt(info / total_bins)
        for h in range(halves):
            slot = pl.ds((b * halves + h) * own, own)
            value = scaled_ref[slot, :] * (x[slot.start:slot.start + own] * strs) / root
            for q in range(own):
                contribution_ref[b:b + 1, pl.ds(q * FA + h * LANES, LANES)] = value[q:q + 1]
        broadband_ref[0:1, b:b + 1] = signal / jnp.sqrt(info)
        broadband_ref[1:2, b:b + 1] = root


def local(strain, valid, intersection, notch):
    total_bins = intersection.shape[1]
    devices = lax.axis_size("seg")
    me = lax.axis_index("seg")
    local_bins = total_bins // devices
    pairs = len(baseline_pairs)
    halves = FA // LANES
    own = local_bins // FA
    start = me * local_bins
    inter = lax.dynamic_slice_in_dim(intersection, start, local_bins, 1)
    kept = lax.dynamic_slice_in_dim(notch, start, local_bins, 0).astype(jnp.float32)[None, :]
    scaled = (kept * inter).reshape(pairs, own, halves, LANES).transpose(0, 2, 1, 3)
    scaled = scaled.reshape(pairs * halves * own, LANES)
    x, tail = local_sums(strain, valid, intersection, notch)
    if own != GROUP:
        x = x.reshape(-1, pairs, halves, GROUP, LANES).transpose(1, 2, 0, 3, 4)
        x = x.reshape(pairs, halves, devices, own, LANES).transpose(2, 0, 1, 3, 4)
    terms = exchange(x, tail, devices, me)
    contribution, broadband = pl.pallas_call(
        functools.partial(finish_kernel, own, strain.shape[2], total_bins, len(terms)),
        out_shape=(jax.ShapeDtypeStruct((pairs, local_bins), jnp.float32),
                   jax.ShapeDtypeStruct((2, pairs), jnp.float32)),
        compiler_params=pltpu.CompilerParams(vmem_limit_bytes=4 << 20),
    )(*terms, scaled)
    return (contribution, broadband.T)


def solution(mesh):
    in_specs = (P(None, "seg", None, None, None), P("seg"), P(), P())
    out_specs = (P(None, "seg"), P())
    return jax.shard_map(local, mesh=mesh, in_specs=in_specs, out_specs=out_specs, check_vma=False)
```

```python
import functools
import math

import jax
import jax.numpy as jnp
import numpy as np
from jax import lax
from jax.experimental import pallas as pl
from jax.experimental.pallas import tpu as pltpu
from jax.sharding import PartitionSpec as P

FA = 256
FB = 256
LANES = 128
BLOCK = 16
GROUP = 8


baseline_pairs = ((0, 1), (0, 2), (1, 2))


def dft_table(length):
    counter = np.arange(length)
    angles = (counter[:, None] * counter[None, :] % length).astype(np.float32) * np.float32(2.0 * math.pi / length)
    cos, sin = np.cos(angles), np.sin(angles)
    real = np.concatenate([cos, sin], axis=1).reshape(-1, BLOCK, 2 * length)
    imag = np.concatenate([-sin, cos], axis=1).reshape(-1, BLOCK, 2 * length)
    return jnp.asarray(np.stack([real, imag], axis=1).reshape(2 * length, 2 * length), jnp.bfloat16)


def twiddle(rows, cols):
    phases = np.arange(rows)[:, None] * np.arange(cols)[None, :]
    angles = phases.astype(np.float32) * np.float32(2.0 * math.pi / (rows * cols))
    scale = np.float32(1.0 / math.sqrt(rows * cols))
    return jnp.asarray(np.stack([np.cos(angles) * scale, np.sin(angles) * scale]), jnp.float32)


def kernel(dets, segs, strs, valid_hbm, x_hbm, table_hbm, tw_hbm, inter_hbm, notch_hbm, out_ref, tail_ref,
           valid_ref, xs, table, tw, inter, notch, wide, mid, spec, stats, sem, table_sem):
    trips = segs * strs
    nb = len(baseline_pairs)

    def load(i):
        part = pl.ds(0, 1) if i == 0 else pl.ds(1, trips - 1)
        return pltpu.make_async_copy(x_hbm.at[:, part], xs.at[:, part], sem.at[i])

    others = [pltpu.make_async_copy(a, b, table_sem.at[n]) for n, (a, b) in enumerate(
        [(table_hbm, table), (tw_hbm, tw), (inter_hbm, inter), (notch_hbm, notch), (valid_hbm, valid_ref)])]
    load(0).start()
    for copy in others[:2]:
        copy.start()
    for i in range(1, 2):
        load(i).start()
    for copy in others[2:]:
        copy.start()

    def spectrum(d, i):
        wide[d] = xs[d, i].astype(jnp.float32)
        cols = []
        for h in range(2):
            parts = [wide[d, pl.ds(2 * h + c, FA, stride=4), :] for c in range(2)]
            cols.append(jnp.concatenate(parts, axis=0).astype(jnp.bfloat16))
        data = jnp.concatenate(cols, axis=1)
        first = jnp.dot(table[...], data, preferred_element_type=jnp.float32)
        for r in range(FA // BLOCK):
            rows = pl.ds(r * BLOCK, BLOCK)
            real = first[2 * r * BLOCK:(2 * r + 1) * BLOCK]
            imag = first[(2 * r + 1) * BLOCK:(2 * r + 2) * BLOCK]
            u, v = tw[0, rows, :], tw[1, rows, :]
            mid[d, rows, :FB] = (real * u + imag * v).astype(jnp.bfloat16)
            mid[d, rows, FB:] = (imag * u - real * v).astype(jnp.bfloat16)
        spec[i % 2, d] = lax.dot_general(table[...], mid[d], (((1,), (1,)), ((), ())),
                                         preferred_element_type=jnp.float32)

    def add_stats(i, part):
        s, t = i // strs, i % strs
        for r in range(part * FB // BLOCK // dets, (part + 1) * FB // BLOCK // dets):
            rows = pl.ds(r * BLOCK, BLOCK)
            real = [spec[i % 2, d, pl.ds(2 * r * BLOCK, BLOCK), :] for d in range(dets)]
            imag = [spec[i % 2, d, pl.ds((2 * r + 1) * BLOCK, BLOCK), :] for d in range(dets)]
            pairs = [(d, d) for d in range(dets)] + list(baseline_pairs)
            for n, (j, k) in enumerate(pairs):
                value = real[j] * real[k] + imag[j] * imag[k]
                stats[s, n, rows, :] = value if t == 0 else stats[s, n, rows, :] + value

    for i in range(trips):
        if i < 2:
            load(i).wait()
        if i == 0:
            for copy in others[:2]:
                copy.wait()
        for d in range(dets):
            spectrum(d, i)
            if i:
                add_stats(i - 1, d)
    for d in range(dets):
        add_stats(trips - 1, d)
    for copy in others[2:]:
        copy.wait()
    flags = [valid_ref[s].astype(jnp.float32) for s in range(segs)]

    def combine(g, sums):
        sums = list(sums)
        for h in range(FA // LANES):
            lanes = pl.ds(h * LANES, LANES)
            rows = pl.ds(pl.multiple_of(g * GROUP, GROUP), GROUP)
            bins = pl.ds(g * GROUP * 2 + h, GROUP, stride=2)
            kept = notch[bins, :].astype(jnp.float32)
            power = [[stats[s, d, rows, lanes] for d in range(dets)] for s in range(segs)]
            for b, (i, j) in enumerate(baseline_pairs):
                weights = [flags[s] / (power[s][i] * power[s][j]) for s in range(segs)]
                numer = weights[0] * stats[0, dets + b, rows, lanes]
                weight = weights[0]
                for s in range(1, segs):
                    numer = numer + weights[s] * stats[s, dets + b, rows, lanes]
                    weight = weight + weights[s]
                scaled = kept * inter[bins, b, :]
                sums[b] = sums[b] + scaled * inter[bins, b, :] * weight
                sums[nb + b] = sums[nb + b] + scaled * numer
                out_ref[g, pl.ds((b * 2 + h) * GROUP, GROUP), :] = numer
        return tuple(sums)

    sums = lax.fori_loop(0, FB // GROUP, combine,
                         tuple(jnp.zeros((GROUP, LANES), jnp.float32) for _ in range(2 * nb)), unroll=4)
    tail = jnp.concatenate([jnp.sum(v, axis=0, keepdims=True) for v in sums]
                           + [jnp.zeros((GROUP - 2 * nb, LANES), jnp.float32)], axis=0)
    tail_ref[...] = tail


def local_sums(strain, valid, intersection, notch):
    dets, segs, strs = strain.shape[:3]
    halves = FB // LANES
    x = strain.reshape(dets * segs * strs, 2, FA, halves, LANES).transpose(0, 2, 3, 1, 4)
    x = x.reshape(dets, segs * strs, 2 * FA * halves, LANES)
    inter = intersection.reshape(len(baseline_pairs), -1, LANES).transpose(1, 0, 2)
    kept = notch.reshape(-1, LANES)
    count = dets * segs * strs
    rows = 2 * len(baseline_pairs) * GROUP
    any_spec = pl.BlockSpec(memory_space=pl.ANY)
    vmem = pl.BlockSpec(memory_space=pltpu.VMEM)
    return pl.pallas_call(
        functools.partial(kernel, dets, segs, strs),
        out_shape=(jax.ShapeDtypeStruct((FB // GROUP, rows, LANES), jnp.float32),
                   jax.ShapeDtypeStruct((GROUP, LANES), jnp.float32)),
        in_specs=[any_spec] * 6,
        out_specs=(vmem, vmem),
        scratch_shapes=[
            pltpu.SMEM(valid.shape, jnp.int32),
            pltpu.VMEM(x.shape, jnp.bfloat16),
            pltpu.VMEM((2 * FA, 2 * FA), jnp.bfloat16),
            pltpu.VMEM((2, FA, FB), jnp.float32),
            pltpu.VMEM(inter.shape, jnp.float32),
            pltpu.VMEM(kept.shape, jnp.int32),
            pltpu.VMEM((dets, 2 * FA * halves, LANES), jnp.float32),
            pltpu.VMEM((dets, FA, 2 * FB), jnp.bfloat16),
            pltpu.VMEM((2, dets, 2 * FB, FA), jnp.float32),
            pltpu.VMEM((segs, dets + len(baseline_pairs), FB, FA), jnp.float32),
            pltpu.SemaphoreType.DMA((count,)),
            pltpu.SemaphoreType.DMA((5,)),
        ],
        compiler_params=pltpu.CompilerParams(vmem_limit_bytes=30 << 20),
        cost_estimate=pl.CostEstimate(flops=count * 16 * FA * FA * FB, bytes_accessed=2 * x.size,
                                      transcendentals=0),
    )(*(pltpu.with_memory_space_constraint(v, pltpu.HBM) for v in (valid, x, dft_table(FA), twiddle(FA, FB), inter, kept)))


def exchange(x, tail, devices, me):
    base = 1
    total = jnp.concatenate([x.reshape(-1, LANES), tail])
    count = devices
    while base < devices:
        radix = 2 if base == 1 or devices // base % 4 else 4
        count //= radix
        size = tail.shape[0]
        parts, tail = total[:-size].reshape(count, radix, -1, LANES), total[-size:]
        shift = base * radix == devices
        digit = jnp.bitwise_and(lax.shift_right_logical(me, base.bit_length() - 1), radix - 1)

        def part(k):
            other = jnp.bitwise_and(digit + k, radix - 1) if shift else jnp.bitwise_xor(digit, k)
            own = lax.dynamic_index_in_dim(parts, other, 1, keepdims=False)
            return jnp.concatenate([own.reshape(-1, LANES), tail])

        def partner(i, k):
            at = i // base % radix
            return i + (((at + k) % radix if shift else at ^ k) - at) * base

        terms = [part(0)] + [lax.ppermute(part(k), "seg", [(i, partner(i, k)) for i in range(devices)])
                             for k in (range(1, radix) if shift else range(radix - 1, 0, -1))]
        total = functools.reduce(jnp.add, terms)
        base *= radix
    return terms


def finish_kernel(own, strs, total_bins, count, *refs):
    terms, (scaled_ref, contribution_ref, broadband_ref) = refs[:count], refs[count:]
    pairs = len(baseline_pairs)
    halves = FA // LANES
    size = pairs * halves * own
    x = functools.reduce(jnp.add, [ref[...] for ref in terms])
    totals = jnp.sum(x[size:size + 2 * pairs], axis=1, keepdims=True)
    for b in range(pairs):
        info = totals[b:b + 1] * (strs * strs)
        signal = totals[pairs + b:pairs + b + 1] * strs
        root = jnp.sqrt(info / total_bins)
        for h in range(halves):
            slot = pl.ds((b * halves + h) * own, own)
            value = scaled_ref[slot, :] * (x[slot.start:slot.start + own] * strs) / root
            for q in range(own):
                contribution_ref[b:b + 1, pl.ds(q * FA + h * LANES, LANES)] = value[q:q + 1]
        broadband_ref[0:1, b:b + 1] = signal / jnp.sqrt(info)
        broadband_ref[1:2, b:b + 1] = root


def local(strain, valid, intersection, notch):
    total_bins = intersection.shape[1]
    devices = lax.axis_size("seg")
    me = lax.axis_index("seg")
    local_bins = total_bins // devices
    pairs = len(baseline_pairs)
    halves = FA // LANES
    own = local_bins // FA
    start = me * local_bins
    inter = lax.dynamic_slice_in_dim(intersection, start, local_bins, 1)
    kept = lax.dynamic_slice_in_dim(notch, start, local_bins, 0).astype(jnp.float32)[None, :]
    scaled = (kept * inter).reshape(pairs, own, halves, LANES).transpose(0, 2, 1, 3)
    scaled = scaled.reshape(pairs * halves * own, LANES)
    x, tail = local_sums(strain, valid, intersection, notch)
    if own != GROUP:
        x = x.reshape(-1, pairs, halves, GROUP, LANES).transpose(1, 2, 0, 3, 4)
        x = x.reshape(pairs, halves, devices, own, LANES).transpose(2, 0, 1, 3, 4)
    terms = exchange(x, tail, devices, me)
    contribution, broadband = pl.pallas_call(
        functools.partial(finish_kernel, own, strain.shape[2], total_bins, len(terms)),
        out_shape=(jax.ShapeDtypeStruct((pairs, local_bins), jnp.float32),
                   jax.ShapeDtypeStruct((2, pairs), jnp.float32)),
        compiler_params=pltpu.CompilerParams(vmem_limit_bytes=4 << 20),
    )(*terms, scaled)
    return (contribution, broadband.T)


def solution(mesh):
    in_specs = (P(None, "seg", None, None, None), P("seg"), P(), P())
    out_specs = (P(None, "seg"), P())
    return jax.shard_map(local, mesh=mesh, in_specs=in_specs, out_specs=out_specs, check_vma=False)
```

```python
import functools
import math

import jax
import jax.numpy as jnp
import numpy as np
from jax import lax
from jax.experimental import pallas as pl
from jax.experimental.pallas import tpu as pltpu
from jax.sharding import PartitionSpec as P

FA = 256
FB = 256
LANES = 128
BLOCK = 16
GROUP = 8


baseline_pairs = ((0, 1), (0, 2), (1, 2))


def dft_table(length):
    counter = np.arange(length)
    angles = (counter[:, None] * counter[None, :] % length).astype(np.float32) * np.float32(2.0 * math.pi / length)
    cos, sin = np.cos(angles), np.sin(angles)
    real = np.concatenate([cos, sin], axis=1).reshape(-1, BLOCK, 2 * length)
    imag = np.concatenate([-sin, cos], axis=1).reshape(-1, BLOCK, 2 * length)
    return jnp.asarray(np.stack([real, imag], axis=1).reshape(2 * length, 2 * length), jnp.bfloat16)


def twiddle(rows, cols):
    phases = np.arange(rows)[:, None] * np.arange(cols)[None, :]
    angles = phases.astype(np.float32) * np.float32(2.0 * math.pi / (rows * cols))
    scale = np.float32(1.0 / math.sqrt(rows * cols))
    return jnp.asarray(np.stack([np.cos(angles) * scale, np.sin(angles) * scale]), jnp.float32)


def kernel(dets, segs, strs, valid_hbm, x_hbm, table_hbm, tw_hbm, inter_hbm, notch_hbm, out_ref, tail_ref,
           valid_ref, xs, table, tw, inter, notch, wide, mid, spec, stats, sem, table_sem):
    trips = segs * strs
    nb = len(baseline_pairs)

    def load(i):
        part = pl.ds(0, 1) if i == 0 else pl.ds(1, trips - 1)
        return pltpu.make_async_copy(x_hbm.at[:, part], xs.at[:, part], sem.at[i])

    others = [pltpu.make_async_copy(a, b, table_sem.at[n]) for n, (a, b) in enumerate(
        [(table_hbm, table), (tw_hbm, tw), (inter_hbm, inter), (notch_hbm, notch), (valid_hbm, valid_ref)])]
    load(0).start()
    for copy in others[:2]:
        copy.start()
    for i in range(1, 2):
        load(i).start()
    for copy in others[2:]:
        copy.start()

    def spectrum(d, i):
        wide[d] = xs[d, i].astype(jnp.float32)
        cols = []
        for h in range(2):
            parts = [wide[d, pl.ds(2 * h + c, FA, stride=4), :] for c in range(2)]
            cols.append(jnp.concatenate(parts, axis=0).astype(jnp.bfloat16))
        data = jnp.concatenate(cols, axis=1)
        first = jnp.dot(table[...], data, preferred_element_type=jnp.float32)
        for r in range(FA // BLOCK):
            rows = pl.ds(r * BLOCK, BLOCK)
            real = first[2 * r * BLOCK:(2 * r + 1) * BLOCK]
            imag = first[(2 * r + 1) * BLOCK:(2 * r + 2) * BLOCK]
            u, v = tw[0, rows, :], tw[1, rows, :]
            mid[d, rows, :FB] = (real * u + imag * v).astype(jnp.bfloat16)
            mid[d, rows, FB:] = (imag * u - real * v).astype(jnp.bfloat16)
        spec[i % 2, d] = lax.dot_general(table[...], mid[d], (((1,), (1,)), ((), ())),
                                         preferred_element_type=jnp.float32)

    def add_stats(i, part):
        s, t = i // strs, i % strs
        for r in range(part * FB // BLOCK // dets, (part + 1) * FB // BLOCK // dets):
          for lanes in (pl.ds(h * LANES, LANES) for h in range(FA // LANES)):
            rows = pl.ds(r * BLOCK, BLOCK)
            real = [spec[i % 2, d, pl.ds(2 * r * BLOCK, BLOCK), lanes] for d in range(dets)]
            imag = [spec[i % 2, d, pl.ds((2 * r + 1) * BLOCK, BLOCK), lanes] for d in range(dets)]
            pairs = [(d, d) for d in range(dets)] + list(baseline_pairs)
            for n, (j, k) in enumerate(pairs):
                value = real[j] * real[k] + imag[j] * imag[k]
                stats[s, n, rows, lanes] = value if t == 0 else stats[s, n, rows, lanes] + value

    for i in range(trips):
        if i < 2:
            load(i).wait()
        if i == 0:
            for copy in others[:2]:
                copy.wait()
        for d in range(dets):
            spectrum(d, i)
            if i:
                add_stats(i - 1, d)
    for d in range(dets):
        add_stats(trips - 1, d)
    for copy in others[2:]:
        copy.wait()
    flags = [valid_ref[s].astype(jnp.float32) for s in range(segs)]

    def combine(g, sums):
        sums = list(sums)
        for h in range(FA // LANES):
            lanes = pl.ds(h * LANES, LANES)
            rows = pl.ds(pl.multiple_of(g * GROUP, GROUP), GROUP)
            bins = pl.ds(g * GROUP * 2 + h, GROUP, stride=2)
            kept = notch[bins, :].astype(jnp.float32)
            power = [[stats[s, d, rows, lanes] for d in range(dets)] for s in range(segs)]
            for b, (i, j) in enumerate(baseline_pairs):
                weights = [flags[s] / (power[s][i] * power[s][j]) for s in range(segs)]
                numer = weights[0] * stats[0, dets + b, rows, lanes]
                weight = weights[0]
                for s in range(1, segs):
                    numer = numer + weights[s] * stats[s, dets + b, rows, lanes]
                    weight = weight + weights[s]
                scaled = kept * inter[bins, b, :]
                sums[b] = sums[b] + scaled * inter[bins, b, :] * weight
                sums[nb + b] = sums[nb + b] + scaled * numer
                out_ref[g, pl.ds((b * 2 + h) * GROUP, GROUP), :] = numer
        return tuple(sums)

    sums = lax.fori_loop(0, FB // GROUP, combine,
                         tuple(jnp.zeros((GROUP, LANES), jnp.float32) for _ in range(2 * nb)), unroll=4)
    tail = jnp.concatenate([jnp.sum(v, axis=0, keepdims=True) for v in sums]
                           + [jnp.zeros((GROUP - 2 * nb, LANES), jnp.float32)], axis=0)
    tail_ref[...] = tail


def local_sums(strain, valid, intersection, notch):
    dets, segs, strs = strain.shape[:3]
    halves = FB // LANES
    x = strain.reshape(dets * segs * strs, 2, FA, halves, LANES).transpose(0, 2, 3, 1, 4)
    x = x.reshape(dets, segs * strs, 2 * FA * halves, LANES)
    inter = intersection.reshape(len(baseline_pairs), -1, LANES).transpose(1, 0, 2)
    kept = notch.reshape(-1, LANES)
    count = dets * segs * strs
    rows = 2 * len(baseline_pairs) * GROUP
    any_spec = pl.BlockSpec(memory_space=pl.ANY)
    vmem = pl.BlockSpec(memory_space=pltpu.VMEM)
    return pl.pallas_call(
        functools.partial(kernel, dets, segs, strs),
        out_shape=(jax.ShapeDtypeStruct((FB // GROUP, rows, LANES), jnp.float32),
                   jax.ShapeDtypeStruct((GROUP, LANES), jnp.float32)),
        in_specs=[any_spec] * 6,
        out_specs=(vmem, vmem),
        scratch_shapes=[
            pltpu.SMEM(valid.shape, jnp.int32),
            pltpu.VMEM(x.shape, jnp.bfloat16),
            pltpu.VMEM((2 * FA, 2 * FA), jnp.bfloat16),
            pltpu.VMEM((2, FA, FB), jnp.float32),
            pltpu.VMEM(inter.shape, jnp.float32),
            pltpu.VMEM(kept.shape, jnp.int32),
            pltpu.VMEM((dets, 2 * FA * halves, LANES), jnp.float32),
            pltpu.VMEM((dets, FA, 2 * FB), jnp.bfloat16),
            pltpu.VMEM((2, dets, 2 * FB, FA), jnp.float32),
            pltpu.VMEM((segs, dets + len(baseline_pairs), FB, FA), jnp.float32),
            pltpu.SemaphoreType.DMA((count,)),
            pltpu.SemaphoreType.DMA((5,)),
        ],
        compiler_params=pltpu.CompilerParams(vmem_limit_bytes=30 << 20),
        cost_estimate=pl.CostEstimate(flops=count * 16 * FA * FA * FB, bytes_accessed=2 * x.size,
                                      transcendentals=0),
    )(*(pltpu.with_memory_space_constraint(v, pltpu.HBM) for v in (valid, x, dft_table(FA), twiddle(FA, FB), inter, kept)))


def exchange(x, tail, devices, me):
    base = 1
    total = jnp.concatenate([x.reshape(-1, LANES), tail])
    count = devices
    while base < devices:
        radix = 2 if base == 1 or devices // base % 4 else 4
        count //= radix
        size = tail.shape[0]
        parts, tail = total[:-size].reshape(count, radix, -1, LANES), total[-size:]
        shift = base * radix == devices
        digit = jnp.bitwise_and(lax.shift_right_logical(me, base.bit_length() - 1), radix - 1)

        def part(k):
            other = jnp.bitwise_and(digit + k, radix - 1) if shift else jnp.bitwise_xor(digit, k)
            own = lax.dynamic_index_in_dim(parts, other, 1, keepdims=False)
            return jnp.concatenate([own.reshape(-1, LANES), tail])

        def partner(i, k):
            at = i // base % radix
            return i + (((at + k) % radix if shift else at ^ k) - at) * base

        terms = [part(0)] + [lax.ppermute(part(k), "seg", [(i, partner(i, k)) for i in range(devices)])
                             for k in (range(1, radix) if shift else range(radix - 1, 0, -1))]
        total = functools.reduce(jnp.add, terms)
        base *= radix
    return terms


def finish_kernel(own, strs, total_bins, count, *refs):
    terms, (scaled_ref, contribution_ref, broadband_ref) = refs[:count], refs[count:]
    pairs = len(baseline_pairs)
    halves = FA // LANES
    size = pairs * halves * own
    x = functools.reduce(jnp.add, [ref[...] for ref in terms])
    totals = jnp.sum(x[size:size + 2 * pairs], axis=1, keepdims=True)
    for b in range(pairs):
        info = totals[b:b + 1] * (strs * strs)
        signal = totals[pairs + b:pairs + b + 1] * strs
        root = jnp.sqrt(info / total_bins)
        for h in range(halves):
            slot = pl.ds((b * halves + h) * own, own)
            value = scaled_ref[slot, :] * (x[slot.start:slot.start + own] * strs) / root
            for q in range(own):
                contribution_ref[b:b + 1, pl.ds(q * FA + h * LANES, LANES)] = value[q:q + 1]
        broadband_ref[0:1, b:b + 1] = signal / jnp.sqrt(info)
        broadband_ref[1:2, b:b + 1] = root


def local(strain, valid, intersection, notch):
    total_bins = intersection.shape[1]
    devices = lax.axis_size("seg")
    me = lax.axis_index("seg")
    local_bins = total_bins // devices
    pairs = len(baseline_pairs)
    halves = FA // LANES
    own = local_bins // FA
    start = me * local_bins
    inter = lax.dynamic_slice_in_dim(intersection, start, local_bins, 1)
    kept = lax.dynamic_slice_in_dim(notch, start, local_bins, 0).astype(jnp.float32)[None, :]
    scaled = (kept * inter).reshape(pairs, own, halves, LANES).transpose(0, 2, 1, 3)
    scaled = scaled.reshape(pairs * halves * own, LANES)
    x, tail = local_sums(strain, valid, intersection, notch)
    if own != GROUP:
        x = x.reshape(-1, pairs, halves, GROUP, LANES).transpose(1, 2, 0, 3, 4)
        x = x.reshape(pairs, halves, devices, own, LANES).transpose(2, 0, 1, 3, 4)
    terms = exchange(x, tail, devices, me)
    contribution, broadband = pl.pallas_call(
        functools.partial(finish_kernel, own, strain.shape[2], total_bins, len(terms)),
        out_shape=(jax.ShapeDtypeStruct((pairs, local_bins), jnp.float32),
                   jax.ShapeDtypeStruct((2, pairs), jnp.float32)),
        compiler_params=pltpu.CompilerParams(vmem_limit_bytes=4 << 20),
    )(*terms, scaled)
    return (contribution, broadband.T)


def solution(mesh):
    in_specs = (P(None, "seg", None, None, None), P("seg"), P(), P())
    out_specs = (P(None, "seg"), P())
    return jax.shard_map(local, mesh=mesh, in_specs=in_specs, out_specs=out_specs, check_vma=False)
```
